32 devices in a mesh: row: 8 (over y, x, core), col: 4 (over z).
Axes of the slice: x: 2, y: 2, z: 4, core: 2. Of those that a mesh axis runs over, the one named last changes fastest.
Arguments:
- tokens: bfloat16 [256, 8192], P('row', 'col'), may hold values from -6 to 6
- gate_codes: int32 [1024, 28672], P('col', 'row'), may hold values from -2147483648 to 2147483646
- up_codes: int32 [1024, 28672], P('col', 'row'), may hold values from -2147483648 to 2147483646
- down_codes: int32 [3584, 8192], P('row', 'col'), may hold values from -2147483648 to 2147483646
- gate_scales: bfloat16 [64, 28672], P('row'), may hold values from 0.0009994507 to 0.0049743652
- up_scales: bfloat16 [64, 28672], P('row'), may hold values from 0.0009994507 to 0.0049743652
- down_scales: bfloat16 [8192, 224], P('row'), may hold values from 0.00059890747 to 0.0029907227
Outputs:
- mixed: bfloat16 [256, 8192], P('row', 'col')
The draws below stay inside these ranges and needn't reach their ends.
Inputs may be any that keep to these rules, and one draw needn't show every extreme that they name: Every word of gate_codes, up_codes and down_codes is an arbitrary 32-bit pattern: all sixteen codes occur in every nibble position.
All inputs are finite; a program needn't handle non-finite values.
Results may differ from the reference program's by a relative error of at most 0.025.
Values may be sent and summed in bfloat16 or wider, within the bound.
A program may use at most 192 MiB of HBM per device.

```python
import math
import jax
import jax.numpy as jnp
from jax import lax

D = 8192
FF = 28672
GROUP = 128
TOKENS = 256
N_ROW = 8


def plant(drawn, rng, smallest, high):
    index_at = [jax.random.randint(jax.random.fold_in(rng, axis), (), 0, length) for axis, length in enumerate(drawn.shape)]
    main_axis = drawn.shape.index(max(drawn.shape))
    neighbour = index_at[:main_axis] + [(index_at[main_axis] + 1) % drawn.shape[main_axis]] + index_at[main_axis + 1:]
    return drawn.at[tuple(index_at)].set(smallest).at[tuple(neighbour)].set(high)


def level_of(rng, dims, pieces, least, high):
    def one(dim, blocks):
        draws = jax.random.uniform(jax.random.fold_in(jax.random.fold_in(rng, 6), dim), (blocks,), jnp.float32, least / len(pieces), high / len(pieces))
        return jnp.repeat(jnp.exp(draws), dims[dim] // blocks).reshape((-1,) + (1,) * (len(dims) - dim - 1))

    gain = one(*pieces[0])
    for cut in pieces[1:]:
        gain = gain * one(*cut)
    return gain


def gaussian(rng, extent, deviation, bound, shards=(), held_as=jnp.bfloat16):
    result = jax.random.normal(rng, extent, jnp.float32) * deviation
    if len(shards) > 0:
        result = level_of(rng, extent, shards, -0.22, 0.18) * result
    return jnp.clip(result, min=-bound, max=bound).astype(held_as)


def setup_inputs(seed: int = 0) -> dict:
    streams_of = jax.random.split(jax.random.key(seed), 8)
    return {
        "tokens": gaussian(streams_of[0], (TOKENS, D), 1.0, 6.0, ((0, 8), (1, 4))),
        "gate_codes": plant(jax.random.randint(streams_of[1], (D // 8, FF), -2147483648, 2147483647), jax.random.fold_in(streams_of[1], 1), -2147483648, 2147483646).astype(jnp.int32),
        "up_codes": plant(jax.random.randint(streams_of[2], (D // 8, FF), -2147483648, 2147483647), jax.random.fold_in(streams_of[2], 1), -2147483648, 2147483646).astype(jnp.int32),
        "down_codes": plant(jax.random.randint(streams_of[3], (FF // 8, D), -2147483648, 2147483647), jax.random.fold_in(streams_of[3], 1), -2147483648, 2147483646).astype(jnp.int32),
        "gate_scales": jnp.clip(jnp.exp(math.log(0.0049743652) - 1.6048472 * jax.random.uniform(streams_of[4], (D // GROUP, FF), jnp.float32) ** level_of(streams_of[4], (D // GROUP, FF), ((0, 8),), -0.2, 0.2)), 0.0009994507, 0.0049743652).astype(jnp.bfloat16),
        "up_scales": jnp.clip(jnp.exp(math.log(0.0049743652) - 1.6048472 * jax.random.uniform(streams_of[5], (D // GROUP, FF), jnp.float32) ** level_of(streams_of[5], (D // GROUP, FF), ((0, 8),), -0.2, 0.2)), 0.0009994507, 0.0049743652).astype(jnp.bfloat16),
        "down_scales": jnp.clip(jnp.exp(math.log(0.0029907227) - 1.6081632 * jax.random.uniform(streams_of[6], (D, FF // GROUP), jnp.float32) ** level_of(streams_of[6], (D, FF // GROUP), ((0, 8),), -0.2, 0.2)), 0.00059890747, 0.0029907227).astype(jnp.bfloat16),
    }


def unpack_codes(packed):
    nibbles = [jnp.bitwise_and(jnp.right_shift(packed, 4 * offset), 15) for offset in range(8)]
    stacked = jnp.stack(nibbles, axis=1)
    return stacked.reshape(packed.shape[0] * 8, packed.shape[1]) - 8


def dequantize_rows(packed, scale_rows, group_size):
    values = unpack_codes(packed).astype(jnp.float32)
    columns = values.shape[1]
    shaped = values.reshape(scale_rows.shape[0], group_size, columns) * scale_rows.astype(jnp.float32)[:, None, :]
    return shaped.reshape(values.shape[0], columns).astype(jnp.bfloat16)


def split_cols(array):
    return array.reshape(array.shape[0], N_ROW, array.shape[1] // N_ROW).transpose(1, 0, 2)


def reference(tokens, gate_codes, up_codes, down_codes, gate_scales, up_scales, down_scales):
    down_blocks = down_codes.reshape(N_ROW, down_codes.shape[0] // N_ROW, D)

    def one_block(running, inputs):
        gate_packed, up_packed, gate_scale, up_scale, down_packed, down_scale = inputs
        gate_sum = jnp.dot(tokens, dequantize_rows(gate_packed, gate_scale, GROUP), preferred_element_type=jnp.float32)
        up_sum = jnp.dot(tokens, dequantize_rows(up_packed, up_scale, GROUP), preferred_element_type=jnp.float32)
        hidden = (jax.nn.silu(gate_sum) * up_sum).astype(jnp.bfloat16)
        partial_value = jnp.dot(hidden, dequantize_rows(down_packed, down_scale.T, GROUP), preferred_element_type=jnp.float32).astype(jnp.bfloat16)
        return running + partial_value.astype(jnp.float32), None

    start_sum = jnp.zeros((tokens.shape[0], D), jnp.float32)
    running, unused = lax.scan(one_block, start_sum, (split_cols(gate_codes), split_cols(up_codes), split_cols(gate_scales), split_cols(up_scales), down_blocks, split_cols(down_scales)))
    return running.astype(jnp.bfloat16)
```

```python
import functools

import jax
import jax.numpy as jnp
from jax import lax
from jax.experimental import pallas as pl
from jax.experimental.pallas import tpu as pltpu
from jax.sharding import PartitionSpec as P

GROUP = 128
PACK = 8
SUB = GROUP // PACK
MESH = pl.DeviceIdType.MESH
DMA = pltpu.SemaphoreType.DMA
S_LAG = 2
H_LAG = 2
FLIP = -2004318072


def permutation():
    source = lax.broadcasted_iota(jnp.int32, (GROUP, GROUP), 0)
    target = lax.broadcasted_iota(jnp.int32, (GROUP, GROUP), 1)
    wanted = lax.rem(target, SUB) * PACK + lax.div(target, SUB)
    return (source == wanted).astype(jnp.bfloat16)


def pieces_of(chunks):
    bounds = sorted({0, max(1, chunks // 7), max(1, 3 * chunks // 7), chunks})
    return list(zip(bounds[:-1], bounds[1:]))


def nibbles(word, k):
    code = word if k == PACK - 1 else jnp.left_shift(word, 28 - 4 * k)
    return jnp.right_shift(code, 28).astype(jnp.float32)


def layer_kernel(
    rows, cols, chunks,
    tokens, gate, up, down, gate_scale, up_scale, down_scale, out,
    all_tokens, moved, gate_codes, up_codes, down_codes,
    gate_got, up_got, down_got, unit_scale, down_rows,
    dense, dense_down, sums, got, hidden, acc,
    half_send, half_got, comb, final_got,
    local_sem, token_send, token_recv, relay_send, relay_recv,
    scale_send, scale_recv, down_send, down_recv,
    sum_send, sum_recv, hid_send, hid_recv,
    half_ssem, half_rsem, final_ssem, final_rsem,
):
    row, col = lax.axis_index("row"), lax.axis_index("col")
    core = lax.rem(row, 2)
    chip = row - core
    sibling = row + 1 - 2 * core
    chips = rows // 2
    share = rows // cols
    last = cols - 1
    count, model = tokens.shape
    total_tokens = count * rows
    half = total_tokens // 2
    width = gate.shape[1]
    lines = gate_scale.shape[0]
    groups = share * lines
    pair = 2 if chunks % 2 == 0 else 1
    pieces = pieces_of(chunks)
    home = lax.div(row, share) == col
    slot = lax.rem(row, share)
    exact = chips & (chips - 1) == 0

    def other(j):
        if not exact:
            return lax.rem(chip + 2 * j, rows)
        peer, bit = chip, 2
        while bit <= 2 * j:
            if (2 * j) & bit:
                peer = peer + bit - 2 * bit * lax.rem(lax.div(chip, bit), 2)
            bit *= 2
        return peer

    def back(j):
        return j if exact else (chips - j) % chips

    def block(side, j):
        return pl.ds(pl.multiple_of((side * chips + j) * count, count), count)

    def remote(source, target, send, recv, **where):
        return pltpu.make_async_remote_copy(
            src_ref=source, dst_ref=target, send_sem=send, recv_sem=recv,
            device_id=where, device_id_type=MESH,
        )

    own_copy = pltpu.make_async_copy(tokens, all_tokens.at[block(core, 0)], local_sem.at[0])
    own_copy.start()

    def code_copies(i):
        first, end = pieces[i]
        at = pl.ds(first * GROUP, (end - first) * GROUP)
        return [
            pltpu.make_async_copy(gate.at[:, at], gate_codes.at[:, at], local_sem.at[2 + 2 * i]),
            pltpu.make_async_copy(up.at[:, at], up_codes.at[:, at], local_sem.at[3 + 2 * i]),
        ]

    for copy in code_copies(0):
        copy.start()

    barrier = pltpu.get_barrier_semaphore()
    for step in range(1, rows):
        pl.semaphore_signal(
            barrier, inc=1, device_id={"row": lax.rem(row + step, rows)}, device_id_type=MESH
        )

    @pl.when(col > 0)
    def _():
        pl.semaphore_signal(barrier, inc=1, device_id={"col": col - 1}, device_id_type=MESH)

    @pl.when(col < last)
    def _():
        pl.semaphore_signal(barrier, inc=1, device_id={"col": col + 1}, device_id_type=MESH)

    inner = jnp.logical_and(col > 0, col < last)

    @pl.when(inner)
    def _():
        pl.semaphore_wait(barrier, rows + 1)

    @pl.when(jnp.logical_not(inner))
    def _():
        pl.semaphore_wait(barrier, rows)

    def scale_copy(kind, i, step):
        first, end = pieces[i]
        peer = lax.rem(row + step, rows)
        span = (end - first) * GROUP
        source, target = ((gate_scale, gate_got), (up_scale, up_got))[kind]
        source = source.at[:, pl.ds(pl.multiple_of(peer * width + first * GROUP, GROUP), span)]
        target = target.at[slot, :, pl.ds(first * GROUP, span)]
        if step == 0:
            return pltpu.make_async_copy(source, target, scale_recv.at[kind, i, slot])
        return remote(
            source, target, scale_send.at[kind, i, step], scale_recv.at[kind, i, slot], row=peer
        )

    def down_copy(step):
        peer = lax.rem(row + step, rows)
        if step == 0:
            return pltpu.make_async_copy(
                down_scale.at[peer], down_got.at[slot], down_recv.at[slot]
            )
        return remote(
            down_scale.at[peer], down_got.at[slot], down_send.at[step], down_recv.at[slot], row=peer
        )

    def start_scales(i):
        @pl.when(home)
        def _():
            for step in range(rows):
                for kind in range(2):
                    scale_copy(kind, i, step).start()

    def wait_slot(copy_of, t, finish):
        here = row == col * share + t

        @pl.when(here)
        def _():
            copy_of(0).wait()

        @pl.when(jnp.logical_not(here))
        def _():
            finish().wait_recv()

    def wait_scales(i):
        first, end = pieces[i]
        at = pl.ds(first * GROUP, (end - first) * GROUP)
        peer = lax.rem(row + 1, rows)
        for t in range(share):
            for kind, target in enumerate((gate_got, up_got)):
                source = (gate_scale, up_scale)[kind]
                wait_slot(
                    lambda step: scale_copy(kind, i, step),
                    t,
                    lambda: remote(
                        source.at[:, at], target.at[t, :, at], scale_send.at[kind, i, 1],
                        scale_recv.at[kind, i, t], row=peer,
                    ),
                )

    def wait_down():
        peer = lax.rem(row + 1, rows)
        span = down_got.shape[2]
        for t in range(share):
            wait_slot(
                down_copy,
                t,
                lambda: remote(
                    down_scale.at[0], down_got.at[t], down_send.at[1], down_recv.at[t], row=peer
                ),
            )
        for t in range(share):
            down_rows[:, t * span : (t + 1) * span] = down_got[t].astype(jnp.float32)

    def token_copy(j, target):
        return remote(
            all_tokens.at[block(core, 0)], all_tokens.at[block(core, target)],
            token_send.at[j], token_recv.at[target], row=other(j) + core,
        )

    def relay(j):
        return remote(
            all_tokens.at[block(core, j)], all_tokens.at[block(core, j)],
            relay_send.at[j], relay_recv.at[j], row=sibling,
        )

    start_scales(0)
    own_copy.wait()
    for j in range(chips - 1, 0, -1):
        token_copy(j, back(j)).start()
    relay(0).start()
    for i in range(1, len(pieces)):
        start_scales(i)
        for copy in code_copies(i):
            copy.start()

    @pl.when(home)
    def _():
        for step in range(rows):
            down_copy(step).start()

    down_load = pltpu.make_async_copy(down, down_codes, local_sem.at[1])
    down_load.start()
    acc[...] = jnp.zeros_like(acc)
    for j in range(1, chips):
        token_copy(back(j), j).wait_recv()
        relay(j).start()
    for j in range(chips):
        relay(j).wait_recv()

    rows_step = min(total_tokens, 256)
    perm = permutation()

    def permute(i, carry):
        lines_at = pl.ds(pl.multiple_of(i * rows_step, rows_step), rows_step)
        for group in range(model // GROUP):
            at = pl.ds(group * GROUP, GROUP)
            moved[lines_at, at] = jnp.dot(
                all_tokens[lines_at, at], perm, preferred_element_type=jnp.float32
            ).astype(jnp.bfloat16)
        return carry

    lax.fori_loop(0, total_tokens // rows_step, permute, 0)

    batch = 4 if groups % 4 == 0 else 1

    def compute(t):
        at = pl.ds(pl.multiple_of(t * GROUP, GROUP), GROUP)
        for kind, (codes, scale) in enumerate(((gate_codes, gate_got), (up_codes, up_got))):
            for s in range(share):
                unit_scale[kind, s * lines : (s + 1) * lines, :] = scale[s, :, at].astype(jnp.float32)

        def one(b, carry):
            for kind, codes in enumerate((gate_codes, up_codes)):
                word = codes[pl.ds(pl.multiple_of(b * batch * SUB, SUB), batch * SUB), at] ^ FLIP
                word = word.reshape(batch, SUB, GROUP)
                scale = jnp.stack(
                    [unit_scale[kind, pl.ds(b * batch + i, 1), :] for i in range(batch)]
                )
                for k in range(PACK):
                    value = (nibbles(word, k) * scale).astype(jnp.bfloat16)
                    dense[pl.ds(b * batch, batch), k, :, kind * GROUP : (kind + 1) * GROUP] = value
            return carry

        lax.fori_loop(0, groups // batch, one, 0)

        def multiply(i, carry):
            lines_at = pl.ds(pl.multiple_of(i * rows_step, rows_step), rows_step)
            total = jnp.dot(
                moved[lines_at, :],
                dense[...].reshape(model, 2 * GROUP),
                preferred_element_type=jnp.float32,
            )
            sums[t, lines_at, :] = total.astype(jnp.bfloat16)
            return carry

        lax.fori_loop(0, total_tokens // rows_step, multiply, 0)

    def side_rows(side):
        return pl.ds(side * half, half)

    def sum_copy(side, q, source, peer):
        return remote(
            source, got.at[side, q], sum_send.at[side, q], sum_recv.at[side, q], col=peer
        )

    def hid_copy(side, q, peer):
        ref = hidden.at[q, side_rows(side)]
        return remote(ref, ref, hid_send.at[side, q], hid_recv.at[side, q], col=peer)

    before, after = jnp.maximum(col - 1, 0), jnp.minimum(col + 1, last)
    any_peer = jnp.where(col == last, col - 1, col + 1)
    sides = ((col, after, before), (last - col, before, after))

    def dequantize_down(p):
        for i in range(pair):
            group = p * pair + i
            word = down_codes[pl.ds(pl.multiple_of(group * SUB, SUB), SUB), :] ^ FLIP
            scale = down_rows[pl.ds(group, 1), :]
            for k in range(PACK):
                dense_down[i, k] = (nibbles(word, k) * scale).astype(jnp.bfloat16)

    columns = 512 if model % 512 == 0 else GROUP

    def multiply_down(p):
        def one(i, carry):
            lines_at = pl.ds(pl.multiple_of(i * rows_step, rows_step), rows_step)
            left = jnp.concatenate(
                [hidden[p * pair + c, lines_at, :] for c in range(pair)], axis=1
            )
            for n in range(0, model, columns):
                at = pl.ds(n, columns)
                acc[lines_at, at] += jnp.dot(
                    left,
                    dense_down[:, :, :, at].reshape(pair * GROUP, columns),
                    preferred_element_type=jnp.float32,
                )
            return carry

        lax.fori_loop(0, total_tokens // rows_step, one, 0)

    drain = last * (S_LAG + H_LAG)

    def tick(t, carry):
        for i, (first, end) in enumerate(pieces):
            @pl.when(t == first)
            def _():
                for copy in code_copies(i):
                    copy.wait()
                wait_scales(i)

        @pl.when(t < chunks)
        def _():
            compute(t)
            for side, (hops, onward, backward) in enumerate(sides):
                @pl.when(hops == 0)
                def _():
                    sum_copy(side, t, sums.at[t, side_rows(side)], onward).start()

        for side, (hops, onward, backward) in enumerate(sides):
            q = t - S_LAG * hops

            @pl.when((hops > 0) & (q >= 0) & (q < chunks))
            def _():
                sum_copy(side, q, got.at[side, q], any_peer).wait_recv()
                total = got[side, q].astype(jnp.float32) + sums[
                    q, side_rows(side), :
                ].astype(jnp.float32)

                @pl.when(hops < last)
                def _():
                    got[side, q] = total.astype(jnp.bfloat16)
                    sum_copy(side, q, got.at[side, q], onward).start()

                @pl.when(hops == last)
                def _():
                    value = jax.nn.silu(total[:, :GROUP]) * total[:, GROUP:]
                    hidden[q, side_rows(side), :] = jnp.dot(
                        value.astype(jnp.bfloat16), perm, preferred_element_type=jnp.float32
                    ).astype(jnp.bfloat16)
                    hid_copy(side, q, backward).start()

        done = t - drain
        active = jnp.logical_and(done >= 0, lax.rem(done + pair, pair) == pair - 1)

        @pl.when(done == 0)
        def _():
            down_load.wait()
            wait_down()

        @pl.when(active)
        def _():
            dequantize_down(lax.div(done, pair))

        for side, (hops, onward, backward) in enumerate(sides):
            left = last - hops
            q = t - S_LAG * last - H_LAG * left

            @pl.when((left > 0) & (q >= 0) & (q < chunks))
            def _():
                hid_copy(side, q, any_peer).wait_recv()

                @pl.when(left < last)
                def _():
                    hid_copy(side, q, backward).start()

        @pl.when(active)
        def _():
            multiply_down(lax.div(done, pair))

        return carry

    lax.fori_loop(0, chunks + drain, tick, 0)

    def half_copy(j):
        return remote(
            half_send.at[j], half_got.at[j], half_ssem.at[j], half_rsem.at[j], row=sibling
        )

    def final_copy(j, target):
        return remote(
            comb.at[j], final_got.at[target], final_ssem.at[j], final_rsem.at[target],
            row=other(j) + core,
        )

    for j in range(chips - 1, -1, -1):
        half_send[j] = acc[block(1 - core, j), :].astype(jnp.bfloat16)
        half_copy(j).start()
    for j in range(chips - 1, 0, -1):
        half_copy(j).wait_recv()
        comb[j] = (acc[block(core, j), :] + half_got[j].astype(jnp.float32)).astype(jnp.bfloat16)
        final_copy(j, back(j)).start()
    half_copy(0).wait_recv()
    total = acc[block(core, 0), :] + half_got[0].astype(jnp.float32)
    for j in range(1, chips):
        final_copy(back(j), j).wait_recv()
        total = total + final_got[j].astype(jnp.float32)
    out[...] = total.astype(jnp.bfloat16)

    for j in range(1, chips):
        token_copy(j, back(j)).wait_send()
        final_copy(j, back(j)).wait_send()
    for j in range(chips):
        relay(j).wait_send()
        half_copy(j).wait_send()

    @pl.when(home)
    def _():
        for step in range(1, rows):
            for i in range(len(pieces)):
                for kind in range(2):
                    scale_copy(kind, i, step).wait_send()
            down_copy(step).wait_send()

    def sent(q, carry):
        for side, (hops, onward, backward) in enumerate(sides):
            @pl.when(hops < last)
            def _():
                sum_copy(side, q, got.at[side, q], any_peer).wait_send()

            @pl.when(hops > 0)
            def _():
                hid_copy(side, q, any_peer).wait_send()

        return carry

    lax.fori_loop(0, chunks, sent, 0)


def layer(tokens, gate, up, down, gate_scale, up_scale, down_scale, rows, cols):
    count, model = tokens.shape
    words, width = gate.shape
    lines = gate_scale.shape[0]
    share = rows // cols
    down_groups = down_scale.shape[1] // rows
    span = down_scale.shape[0]
    down_scale = down_scale.T.reshape(rows, down_groups, span)
    chunks = width // GROUP
    chips = rows // 2
    tokens_all = count * rows
    half = tokens_all // 2
    groups = share * lines
    pair = 2 if chunks % 2 == 0 else 1
    parts = len(pieces_of(chunks))
    any_spec = pl.BlockSpec(memory_space=pl.ANY)
    bf16, f32, i32 = jnp.bfloat16, jnp.float32, jnp.int32
    return pl.pallas_call(
        functools.partial(layer_kernel, rows, cols, chunks),
        in_specs=[any_spec] * 7,
        out_specs=pl.BlockSpec(memory_space=pltpu.VMEM),
        out_shape=jax.ShapeDtypeStruct((count, model), bf16),
        scratch_shapes=[
            pltpu.VMEM((tokens_all, model), bf16),
            pltpu.VMEM((tokens_all, model), bf16),
            pltpu.VMEM((words, width), i32),
            pltpu.VMEM((words, width), i32),
            pltpu.VMEM(down.shape, i32),
            pltpu.VMEM((share, lines, width), bf16),
            pltpu.VMEM((share, lines, width), bf16),
            pltpu.VMEM((share, down_groups, span), bf16),
            pltpu.VMEM((2, groups, GROUP), f32),
            pltpu.VMEM((down_groups, share * span), f32),
            pltpu.VMEM((groups, PACK, SUB, 2 * GROUP), bf16),
            pltpu.VMEM((pair, PACK, SUB, model), bf16),
            pltpu.VMEM((chunks, tokens_all, 2 * GROUP), bf16),
            pltpu.VMEM((2, chunks, half, 2 * GROUP), bf16),
            pltpu.VMEM((chunks, tokens_all, GROUP), bf16),
            pltpu.VMEM((tokens_all, model), f32),
            pltpu.VMEM((chips, count, model), bf16),
            pltpu.VMEM((chips, count, model), bf16),
            pltpu.VMEM((chips, count, model), bf16),
            pltpu.VMEM((chips, count, model), bf16),
            DMA((2 + 2 * parts,)),
            DMA((chips,)),
            DMA((chips,)),
            DMA((chips,)),
            DMA((chips,)),
            DMA((2, parts, rows)),
            DMA((2, parts, share)),
            DMA((rows,)),
            DMA((share,)),
            DMA((2, chunks)),
            DMA((2, chunks)),
            DMA((2, chunks)),
            DMA((2, chunks)),
            DMA((chips,)),
            DMA((chips,)),
            DMA((chips,)),
            DMA((chips,)),
        ],
        compiler_params=pltpu.CompilerParams(
            collective_id=0, has_side_effects=True, vmem_limit_bytes=60 * 1024 * 1024
        ),
        name="layer",
    )(tokens, gate, up, down, gate_scale, up_scale, down_scale)


def per_device(tokens, gate_codes, up_codes, down_codes, gate_scales, up_scales, down_scales):
    rows, cols = lax.axis_size("row"), lax.axis_size("col")
    return layer(
        tokens, gate_codes, up_codes, down_codes, gate_scales, up_scales, down_scales, rows, cols
    )


def solution(mesh):
    placed = (
        P("row", "col"),
        P("col", "row"),
        P("col", "row"),
        P("row", "col"),
        P("row", None),
        P("row", None),
        P("row", None),
    )
    return jax.shard_map(
        per_device, mesh=mesh, in_specs=placed, out_specs=P("row", "col"), check_vma=False
    )
```

```python
import functools

import jax
import jax.numpy as jnp
from jax import lax
from jax.experimental import pallas as pl
from jax.experimental.pallas import tpu as pltpu
from jax.sharding import PartitionSpec as P

GROUP = 128
PACK = 8
SUB = GROUP // PACK
MESH = pl.DeviceIdType.MESH
DMA = pltpu.SemaphoreType.DMA
S_LAG = 3
H_LAG = 3
H_WAIT = 4
FLIP = -2004318072


def permutation():
    source = lax.broadcasted_iota(jnp.int32, (GROUP, GROUP), 0)
    target = lax.broadcasted_iota(jnp.int32, (GROUP, GROUP), 1)
    wanted = lax.rem(target, SUB) * PACK + lax.div(target, SUB)
    return (source == wanted).astype(jnp.bfloat16)


def pieces_of(chunks):
    bounds = sorted({0, max(1, chunks // 7), max(1, 3 * chunks // 7), chunks})
    return list(zip(bounds[:-1], bounds[1:]))


def nibbles(word, k):
    code = word if k == PACK - 1 else jnp.left_shift(word, 28 - 4 * k)
    return jnp.right_shift(code, 28).astype(jnp.float32)


def layer_kernel(
    rows, cols, chunks,
    tokens, gate, up, down, gate_scale, up_scale, down_scale, out,
    all_tokens, moved, gate_codes, up_codes, down_codes,
    gate_own, up_own, down_own, down_turned,
    gate_got, up_got, down_got, unit_scale, down_rows,
    dense, dense_down, sums, got, hidden_far, hidden_near, acc_far, acc_near,
    half_send, half_got, comb, final_got,
    local_sem, token_send, token_recv, relay_send, relay_recv,
    scale_send, scale_recv, down_send, down_recv,
    sum_send, sum_recv, hid_send, hid_recv,
    half_ssem, half_rsem, final_ssem, final_rsem,
):
    row, col = lax.axis_index("row"), lax.axis_index("col")
    core = lax.rem(row, 2)
    chip = row - core
    sibling = row + 1 - 2 * core
    chips = rows // 2
    share = rows // cols
    last = cols - 1
    count, model = tokens.shape
    total_tokens = count * rows
    half = total_tokens // 2
    width = gate.shape[1]
    lines = gate_scale.shape[0]
    groups = share * lines
    far = half - count
    pair, quad = 2 - chunks % 2, 4 if chunks % 4 == 0 else 1
    pieces = pieces_of(chunks)
    home = lax.div(row, share) == col
    slot = lax.rem(row, share)
    exact = chips & (chips - 1) == 0

    def other(j):
        if not exact:
            return lax.rem(chip + 2 * j, rows)
        peer, bit = chip, 2
        while bit <= 2 * j:
            if (2 * j) & bit:
                peer = peer + bit - 2 * bit * lax.rem(lax.div(chip, bit), 2)
            bit *= 2
        return peer

    def back(j):
        return j if exact else (chips - j) % chips

    def block(side, j):
        return pl.ds(pl.multiple_of((side * chips + j) * count, count), count)

    def remote(source, target, send, recv, **where):
        return pltpu.make_async_remote_copy(
            src_ref=source, dst_ref=target, send_sem=send, recv_sem=recv,
            device_id=where, device_id_type=MESH,
        )

    own_copy = pltpu.make_async_copy(tokens, all_tokens.at[block(core, 0)], local_sem.at[0])
    own_copy.start()

    def code_copies(i):
        first, end = pieces[i]
        at = pl.ds(first * GROUP, (end - first) * GROUP)
        return [
            pltpu.make_async_copy(gate.at[:, at], gate_codes.at[:, at], local_sem.at[2 + 2 * i]),
            pltpu.make_async_copy(up.at[:, at], up_codes.at[:, at], local_sem.at[3 + 2 * i]),
        ]

    for copy in code_copies(0):
        copy.start()
    first_code = 2 + 2 * len(pieces)
    scale_loads = [
        pltpu.make_async_copy(source, target, local_sem.at[first_code + i])
        for i, (source, target) in enumerate(
            ((gate_scale, gate_own), (up_scale, up_own), (down_scale, down_own))
        )
    ]

    @pl.when(home)
    def _():
        for load in scale_loads:
            load.start()

    barrier = pltpu.get_barrier_semaphore()
    for step in range(1, rows):
        pl.semaphore_signal(
            barrier, inc=1, device_id={"row": lax.rem(row + step, rows)}, device_id_type=MESH
        )

    @pl.when(col > 0)
    def _():
        pl.semaphore_signal(barrier, inc=1, device_id={"col": col - 1}, device_id_type=MESH)

    @pl.when(col < last)
    def _():
        pl.semaphore_signal(barrier, inc=1, device_id={"col": col + 1}, device_id_type=MESH)

    inner = jnp.logical_and(col > 0, col < last)

    @pl.when(inner)
    def _():
        pl.semaphore_wait(barrier, rows + 1)

    @pl.when(jnp.logical_not(inner))
    def _():
        pl.semaphore_wait(barrier, rows)

    def scale_copy(kind, i, step):
        first, end = pieces[i]
        peer = lax.rem(row + step, rows)
        span = (end - first) * GROUP
        source, target = ((gate_own, gate_got), (up_own, up_got))[kind]
        source = source.at[:, pl.ds(pl.multiple_of(peer * width + first * GROUP, GROUP), span)]
        target = target.at[slot, :, pl.ds(first * GROUP, span)]
        if step == 0:
            return pltpu.make_async_copy(source, target, scale_recv.at[kind, i, slot])
        return remote(
            source, target, scale_send.at[kind, i, step], scale_recv.at[kind, i, slot], row=peer
        )

    def down_copy(step):
        peer = lax.rem(row + step, rows)
        if step == 0:
            return pltpu.make_async_copy(
                down_turned.at[peer], down_got.at[slot], down_recv.at[slot]
            )
        return remote(
            down_turned.at[peer], down_got.at[slot], down_send.at[step], down_recv.at[slot], row=peer
        )

    def start_scales(i):
        @pl.when(home)
        def _():
            for step in range(rows):
                for kind in range(2):
                    scale_copy(kind, i, step).start()

    def wait_slot(copy_of, t, finish):
        here = row == col * share + t

        @pl.when(here)
        def _():
            copy_of(0).wait()

        @pl.when(jnp.logical_not(here))
        def _():
            finish().wait_recv()

    def wait_scales(i):
        first, end = pieces[i]
        at = pl.ds(first * GROUP, (end - first) * GROUP)
        peer = lax.rem(row + 1, rows)
        for t in range(share):
            for kind, target in enumerate((gate_got, up_got)):
                source = (gate_own, up_own)[kind]
                wait_slot(
                    lambda step: scale_copy(kind, i, step),
                    t,
                    lambda: remote(
                        source.at[:, at], target.at[t, :, at], scale_send.at[kind, i, 1],
                        scale_recv.at[kind, i, t], row=peer,
                    ),
                )

    def wait_down():
        peer = lax.rem(row + 1, rows)
        span = down_got.shape[2]
        for t in range(share):
            wait_slot(
                down_copy,
                t,
                lambda: remote(
                    down_turned.at[0], down_got.at[t], down_send.at[1], down_recv.at[t], row=peer
                ),
            )
        for t in range(share):
            down_rows[:, t * span : (t + 1) * span] = down_got[t].astype(jnp.float32)

    def token_copy(j, target):
        return remote(
            all_tokens.at[block(core, 0)], all_tokens.at[block(core, target)],
            token_send.at[j], token_recv.at[target], row=other(j) + core,
        )

    def relay(j):
        return remote(
            all_tokens.at[block(core, j)], all_tokens.at[block(core, j)],
            relay_send.at[j], relay_recv.at[j], row=sibling,
        )

    @pl.when(home)
    def _():
        for load in scale_loads:
            load.wait()

    start_scales(0)
    own_copy.wait()
    for j in range(chips - 1, 0, -1):
        token_copy(j, back(j)).start()
    relay(0).start()
    for i in range(1, len(pieces)):
        start_scales(i)
        for copy in code_copies(i):
            copy.start()

    @pl.when(home)
    def _():
        down_groups = down_own.shape[1] // rows
        line = lax.broadcasted_iota(jnp.int32, (rows * down_got.shape[1], down_own.shape[1]), 0)
        wanted = lax.broadcasted_iota(jnp.int32, line.shape, 1)
        owner = lax.div(line, down_got.shape[1])
        group = lax.rem(line, down_got.shape[1])
        pick = (wanted == owner * down_groups + group) & (group < down_groups)
        turned = lax.dot_general(
            pick.astype(jnp.bfloat16), down_own[...], (((1,), (1,)), ((), ())),
            preferred_element_type=jnp.float32,
        )
        down_turned[...] = turned.astype(jnp.bfloat16).reshape(down_turned.shape)
        for step in range(rows):
            down_copy(step).start()

    down_load = pltpu.make_async_copy(down, down_codes, local_sem.at[1])
    down_load.start()
    acc_far[...] = jnp.zeros_like(acc_far)
    acc_near[...] = jnp.zeros_like(acc_near)
    for j in range(1, chips):
        token_copy(back(j), j).wait_recv()
        relay(j).start()
    for j in range(chips):
        relay(j).wait_recv()

    rows_step = min(total_tokens, 256)
    perm = permutation()

    def permute(i, carry):
        lines_at = pl.ds(pl.multiple_of(i * rows_step, rows_step), rows_step)
        for group in range(model // GROUP):
            at = pl.ds(group * GROUP, GROUP)
            moved[lines_at, at] = jnp.dot(
                all_tokens[lines_at, at], perm, preferred_element_type=jnp.float32
            ).astype(jnp.bfloat16)
        return carry

    lax.fori_loop(0, total_tokens // rows_step, permute, 0)

    batch = 4 if groups % 4 == 0 else 1

    def compute(t):
        at = pl.ds(pl.multiple_of(t * GROUP, GROUP), GROUP)
        for kind, (codes, scale) in enumerate(((gate_codes, gate_got), (up_codes, up_got))):
            for s in range(share):
                unit_scale[kind, s * lines : (s + 1) * lines, :] = scale[s, :, at].astype(jnp.float32)

        def one(b, carry):
            for kind, codes in enumerate((gate_codes, up_codes)):
                word = codes[pl.ds(pl.multiple_of(b * batch * SUB, SUB), batch * SUB), at] ^ FLIP
                word = word.reshape(batch, SUB, GROUP)
                scale = jnp.stack(
                    [unit_scale[kind, pl.ds(b * batch + i, 1), :] for i in range(batch)]
                )
                for k in range(PACK):
                    value = (nibbles(word, k) * scale).astype(jnp.bfloat16)
                    dense[pl.ds(b * batch, batch), k, :, kind * GROUP : (kind + 1) * GROUP] = value
            return carry

        lax.fori_loop(0, groups // batch, one, 0)

        def multiply(i, carry):
            lines_at = pl.ds(pl.multiple_of(i * rows_step, rows_step), rows_step)
            total = jnp.dot(
                moved[lines_at, :],
                dense[...].reshape(model, 2 * GROUP),
                preferred_element_type=jnp.float32,
            )
            sums[t, lines_at, :] = total.astype(jnp.bfloat16)
            return carry

        lax.fori_loop(0, total_tokens // rows_step, multiply, 0)

    def side_rows(side):
        return pl.ds(side * half, half)

    def sum_copy(side, q, source, peer):
        return remote(
            source, got.at[side, q], sum_send.at[side, q], sum_recv.at[side, q], col=peer
        )

    def far_copy(side, tau, peer):
        ref = hidden_far.at[side, pl.ds(tau * pair, pair)]
        return remote(ref, ref, hid_send.at[side, tau], hid_recv.at[side, tau], col=peer)

    def near_copy(side, tau, peer):
        ref = hidden_near.at[side, pl.ds(tau * quad, quad)]
        at = far_ticks + tau
        return remote(ref, ref, hid_send.at[side, at], hid_recv.at[side, at], col=peer)

    far_ticks, near_ticks = chunks // pair, chunks // quad
    h_start = chunks + last * S_LAG - far_ticks + H_WAIT
    d_start = h_start + last * H_LAG

    before, after = jnp.maximum(col - 1, 0), jnp.minimum(col + 1, last)
    any_peer = jnp.where(col == last, col - 1, col + 1)
    sides = ((col, after, before), (last - col, before, after))

    def dequantize_down(group):
        word = down_codes[pl.ds(pl.multiple_of(group * SUB, SUB), SUB), :] ^ FLIP
        scale = down_rows[pl.ds(group, 1), :]
        for k in range(PACK):
            dense_down[group, k] = (nibbles(word, k) * scale).astype(jnp.bfloat16)

    columns = 512 if model % 512 == 0 else GROUP

    def multiply_down(tau, units, hidden, target):
        depth = target.shape[1]
        cuts = 1
        while (2 * depth if cuts == 1 else depth // (cuts // 2)) > 256:
            cuts *= 2
        for cut in range(cuts):
            if cuts == 1:
                at = (slice(None), slice(None))
                height = 2 * depth
            else:
                height = depth * 2 // cuts
                place = cut % (cuts // 2) * height
                at = (pl.ds(cut // (cuts // 2), 1), pl.ds(place, height))
            left = jnp.concatenate(
                [
                    hidden[at[0], tau * units + c, at[1], :].reshape(height, GROUP)
                    for c in range(units)
                ],
                axis=1,
            )
            for n in range(0, model, columns):
                right = dense_down[pl.ds(tau * units, units), :, :, pl.ds(n, columns)]
                total = jnp.dot(
                    left,
                    right.reshape(units * GROUP, columns),
                    preferred_element_type=jnp.float32,
                )
                lanes = pl.ds(n, columns)
                old = target[at[0], at[1], lanes]
                target[at[0], at[1], lanes] = old + total.reshape(old.shape)

    def half_copy(j):
        return remote(
            half_send.at[j], half_got.at[j], half_ssem.at[j], half_rsem.at[j], row=sibling
        )

    def final_copy(j, target):
        return remote(
            comb.at[j], final_got.at[target], final_ssem.at[j], final_rsem.at[target],
            row=other(j) + core,
        )

    def far_rows(side, j):
        return acc_far[side, (j - 1) * count : j * count, :]

    def tick(t, carry):
        for i, (first, end) in enumerate(pieces):
            @pl.when(t == first)
            def _():
                for copy in code_copies(i):
                    copy.wait()
                wait_scales(i)

        @pl.when(t < chunks)
        def _():
            compute(t)
            for side, (hops, onward, backward) in enumerate(sides):
                @pl.when(hops == 0)
                def _():
                    sum_copy(side, t, sums.at[t, side_rows(side)], onward).start()

        for side, (hops, onward, backward) in enumerate(sides):
            q = t - S_LAG * hops

            @pl.when((hops > 0) & (q >= 0) & (q < chunks))
            def _():
                sum_copy(side, q, got.at[side, q], any_peer).wait_recv()
                total = got[side, q].astype(jnp.float32) + sums[
                    q, side_rows(side), :
                ].astype(jnp.float32)

                @pl.when(hops < last)
                def _():
                    got[side, q] = total.astype(jnp.bfloat16)
                    sum_copy(side, q, got.at[side, q], onward).start()

                @pl.when(hops == last)
                def _():
                    value = jax.nn.silu(total[:, :GROUP]) * total[:, GROUP:]
                    value = jnp.dot(
                        value.astype(jnp.bfloat16), perm, preferred_element_type=jnp.float32
                    ).astype(jnp.bfloat16)
                    hidden_near[side, q] = value[:count]
                    hidden_far[side, q] = value[count:]

        group = t - (d_start - far_ticks)

        @pl.when(group == 0)
        def _():
            down_load.wait()
            wait_down()

        @pl.when((group >= 0) & (group < chunks))
        def _():
            dequantize_down(group)

        for side, (hops, onward, backward) in enumerate(sides):
            left = last - hops
            tau = t - h_start - H_LAG * left

            @pl.when((tau >= 0) & (tau < far_ticks))
            def _():
                @pl.when(left > 0)
                def _():
                    far_copy(side, tau, any_peer).wait_recv()

                @pl.when(left < last)
                def _():
                    far_copy(side, tau, backward).start()

            @pl.when((tau >= far_ticks) & (tau < far_ticks + near_ticks))
            def _():
                @pl.when(left > 0)
                def _():
                    near_copy(side, tau - far_ticks, any_peer).wait_recv()

                @pl.when(left < last)
                def _():
                    near_copy(side, tau - far_ticks, backward).start()

        tau = t - d_start

        @pl.when((tau >= 0) & (tau < far_ticks))
        def _():
            multiply_down(tau, pair, hidden_far, acc_far)

        @pl.when(tau >= far_ticks)
        def _():
            multiply_down(tau - far_ticks, quad, hidden_near, acc_near)

        @pl.when(tau == far_ticks - 1)
        def _():
            for j in range(chips - 1, 0, -1):
                half_send[j] = far_rows(1 - core, j).astype(jnp.bfloat16)
                half_copy(j).start()

        @pl.when(tau == far_ticks + min(1, near_ticks - 1))
        def _():
            for j in range(chips - 1, 0, -1):
                half_copy(j).wait_recv()
                comb[j] = (far_rows(core, j) + half_got[j].astype(jnp.float32)).astype(
                    jnp.bfloat16
                )
                final_copy(j, back(j)).start()

        return carry

    lax.fori_loop(0, d_start + far_ticks + near_ticks, tick, 0)

    half_send[0] = acc_near[1 - core].astype(jnp.bfloat16)
    half_copy(0).start()
    total = acc_near[core]
    for j in range(1, chips):
        final_copy(back(j), j).wait_recv()
        total = total + final_got[j].astype(jnp.float32)
    half_copy(0).wait_recv()
    out[...] = (total + half_got[0].astype(jnp.float32)).astype(jnp.bfloat16)

    for j in range(1, chips):
        token_copy(j, back(j)).wait_send()
        final_copy(j, back(j)).wait_send()
    for j in range(chips):
        relay(j).wait_send()
        half_copy(j).wait_send()

    @pl.when(home)
    def _():
        for step in range(1, rows):
            for i in range(len(pieces)):
                for kind in range(2):
                    scale_copy(kind, i, step).wait_send()
            down_copy(step).wait_send()

    def sent_sums(q, carry):
        for side, (hops, onward, backward) in enumerate(sides):
            @pl.when(hops < last)
            def _():
                sum_copy(side, q, got.at[side, q], any_peer).wait_send()

        return carry

    def sent_hidden(copy_of):
        def one(tau, carry):
            for side, (hops, onward, backward) in enumerate(sides):
                @pl.when(hops > 0)
                def _():
                    copy_of(side, tau, any_peer).wait_send()

            return carry

        return one

    lax.fori_loop(0, chunks, sent_sums, 0)
    lax.fori_loop(0, far_ticks, sent_hidden(far_copy), 0)
    lax.fori_loop(0, near_ticks, sent_hidden(near_copy), 0)


def layer(tokens, gate, up, down, gate_scale, up_scale, down_scale, rows, cols):
    count, model = tokens.shape
    words, width = gate.shape
    lines = gate_scale.shape[0]
    share = rows // cols
    down_groups = down_scale.shape[1] // rows
    span = down_scale.shape[0]
    lines_down = -(-down_groups // 16) * 16
    chunks = width // GROUP
    chips = rows // 2
    tokens_all = count * rows
    half = tokens_all // 2
    groups = share * lines
    pair, quad = 2 - chunks % 2, 4 if chunks % 4 == 0 else 1
    steps = chunks // pair + chunks // quad
    parts = len(pieces_of(chunks))
    any_spec = pl.BlockSpec(memory_space=pl.ANY)
    bf16, f32, i32 = jnp.bfloat16, jnp.float32, jnp.int32
    return pl.pallas_call(
        functools.partial(layer_kernel, rows, cols, chunks),
        in_specs=[any_spec] * 7,
        out_specs=pl.BlockSpec(memory_space=pltpu.VMEM),
        out_shape=jax.ShapeDtypeStruct((count, model), bf16),
        scratch_shapes=[
            pltpu.VMEM((tokens_all, model), bf16),
            pltpu.VMEM((tokens_all, model), bf16),
            pltpu.VMEM((words, width), i32),
            pltpu.VMEM((words, width), i32),
            pltpu.VMEM(down.shape, i32),
            pltpu.VMEM(gate_scale.shape, bf16),
            pltpu.VMEM(up_scale.shape, bf16),
            pltpu.VMEM(down_scale.shape, bf16),
            pltpu.VMEM((rows, lines_down, span), bf16),
            pltpu.VMEM((share, lines, width), bf16),
            pltpu.VMEM((share, lines, width), bf16),
            pltpu.VMEM((share, lines_down, span), bf16),
            pltpu.VMEM((2, groups, GROUP), f32),
            pltpu.VMEM((lines_down, share * span), f32),
            pltpu.VMEM((groups, PACK, SUB, 2 * GROUP), bf16),
            pltpu.VMEM((chunks, PACK, SUB, model), bf16),
            pltpu.VMEM((chunks, tokens_all, 2 * GROUP), bf16),
            pltpu.VMEM((2, chunks, half, 2 * GROUP), bf16),
            pltpu.VMEM((2, chunks, half - count, GROUP), bf16),
            pltpu.VMEM((2, chunks, count, GROUP), bf16),
            pltpu.VMEM((2, half - count, model), f32),
            pltpu.VMEM((2, count, model), f32),
            pltpu.VMEM((chips, count, model), bf16),
            pltpu.VMEM((chips, count, model), bf16),
            pltpu.VMEM((chips, count, model), bf16),
            pltpu.VMEM((chips, count, model), bf16),
            DMA((5 + 2 * parts,)),
            DMA((chips,)),
            DMA((chips,)),
            DMA((chips,)),
            DMA((chips,)),
            DMA((2, parts, rows)),
            DMA((2, parts, share)),
            DMA((rows,)),
            DMA((share,)),
            DMA((2, chunks)),
            DMA((2, chunks)),
            DMA((2, steps)),
            DMA((2, steps)),
            DMA((chips,)),
            DMA((chips,)),
            DMA((chips,)),
            DMA((chips,)),
        ],
        compiler_params=pltpu.CompilerParams(
            collective_id=0, has_side_effects=True, vmem_limit_bytes=60 * 1024 * 1024
        ),
        name="layer",
    )(tokens, gate, up, down, gate_scale, up_scale, down_scale)


def per_device(tokens, gate_codes, up_codes, down_codes, gate_scales, up_scales, down_scales):
    rows, cols = lax.axis_size("row"), lax.axis_size("col")
    return layer(
        tokens, gate_codes, up_codes, down_codes, gate_scales, up_scales, down_scales, rows, cols
    )


def solution(mesh):
    placed = (
        P("row", "col"),
        P("col", "row"),
        P("col", "row"),
        P("row", "col"),
        P("row", None),
        P("row", None),
        P("row", None),
    )
    return jax.shard_map(
        per_device, mesh=mesh, in_specs=placed, out_specs=P("row", "col"), check_vma=False
    )
```

```python
import functools

import jax
import jax.numpy as jnp
from jax import lax
from jax.experimental import pallas as pl
from jax.experimental.pallas import tpu as pltpu
from jax.sharding import PartitionSpec as P

GROUP = 128
PACK = 8
SUB = GROUP // PACK
MESH = pl.DeviceIdType.MESH
DMA = pltpu.SemaphoreType.DMA
S_LAG = 3
H_LAG = 5
H_WAIT = 0
PARTS = 1
EARLY = 2
FLIP = -2004318072


def permutation():
    source = lax.broadcasted_iota(jnp.int32, (GROUP, GROUP), 0)
    target = lax.broadcasted_iota(jnp.int32, (GROUP, GROUP), 1)
    wanted = lax.rem(target, SUB) * PACK + lax.div(target, SUB)
    return (source == wanted).astype(jnp.bfloat16)


def pieces_of(chunks):
    bounds = sorted({0, 1, max(1, chunks // 7), max(1, 3 * chunks // 7), chunks})
    return list(zip(bounds[:-1], bounds[1:]))


def nibbles(word, k):
    code = word if k == PACK - 1 else jnp.left_shift(word, 28 - 4 * k)
    return jnp.right_shift(code, 28).astype(jnp.float32)


def layer_kernel(
    rows, cols, chunks,
    tokens, gate, up, down, gate_scale, up_scale, down_scale, out,
    all_tokens, moved, gate_codes, up_codes, down_codes,
    gate_own, up_own, down_own, down_turned,
    gate_got, up_got, down_got, unit_scale, down_rows,
    dense, dense_down, sums, got,
    hidden, acc,
    half_send, half_got, comb, final_got,
    local_sem, token_send, token_recv, relay_send, relay_recv,
    scale_send, scale_recv, down_recv,
    sum_send, sum_recv, hid_send, hid_recv,
    half_ssem, half_rsem, final_ssem, final_rsem,
):
    row, col = lax.axis_index("row"), lax.axis_index("col")
    core = lax.rem(row, 2)
    chip = row - core
    sibling = row + 1 - 2 * core
    chips = rows // 2
    share = rows // cols
    last = cols - 1
    count, model = tokens.shape
    total_tokens = count * rows
    half = total_tokens // 2
    width = gate.shape[1]
    lines = gate_scale.shape[0]
    groups = share * lines
    part = half // PARTS
    pair, quad = 2 - chunks % 2, 4 if chunks % 4 == 0 else 1
    pieces = pieces_of(chunks)
    home = lax.div(row, share) == col
    slot = lax.rem(row, share)
    exact = chips & (chips - 1) == 0

    def other(j):
        if not exact:
            return lax.rem(chip + 2 * j, rows)
        peer, bit = chip, 2
        while bit <= 2 * j:
            if (2 * j) & bit:
                peer = peer + bit - 2 * bit * lax.rem(lax.div(chip, bit), 2)
            bit *= 2
        return peer

    def back(j):
        return j if exact else (chips - j) % chips

    def block(side, j):
        return pl.ds(pl.multiple_of((side * chips + j) * count, count), count)

    def remote(source, target, send, recv, **where):
        return pltpu.make_async_remote_copy(
            src_ref=source, dst_ref=target, send_sem=send, recv_sem=recv,
            device_id=where, device_id_type=MESH,
        )

    own_copy = pltpu.make_async_copy(tokens, all_tokens.at[block(core, 0)], local_sem.at[0])
    own_copy.start()

    def code_copies(i):
        first, end = pieces[i]
        at = pl.ds(first * GROUP, (end - first) * GROUP)
        return [
            pltpu.make_async_copy(gate.at[:, at], gate_codes.at[:, at], local_sem.at[2 + 2 * i]),
            pltpu.make_async_copy(up.at[:, at], up_codes.at[:, at], local_sem.at[3 + 2 * i]),
        ]

    for copy in code_copies(0):
        copy.start()
    first_code = 2 + 2 * len(pieces)
    scale_loads = [
        pltpu.make_async_copy(source, target, local_sem.at[first_code + i])
        for i, (source, target) in enumerate(
            ((gate_scale, gate_own), (up_scale, up_own), (down_scale, down_own))
        )
    ]

    @pl.when(home)
    def _():
        for load in scale_loads:
            load.start()

    barrier = pltpu.get_barrier_semaphore()
    for step in range(1, rows):
        pl.semaphore_signal(
            barrier, inc=1, device_id={"row": lax.rem(row + step, rows)}, device_id_type=MESH
        )

    @pl.when(col > 0)
    def _():
        pl.semaphore_signal(barrier, inc=1, device_id={"col": col - 1}, device_id_type=MESH)

    @pl.when(col < last)
    def _():
        pl.semaphore_signal(barrier, inc=1, device_id={"col": col + 1}, device_id_type=MESH)

    inner = jnp.logical_and(col > 0, col < last)

    @pl.when(inner)
    def _():
        pl.semaphore_wait(barrier, rows + 1)

    @pl.when(jnp.logical_not(inner))
    def _():
        pl.semaphore_wait(barrier, rows)

    def scale_copy(kind, i, step):
        first, end = pieces[i]
        peer = lax.rem(row + step, rows)
        span = (end - first) * GROUP
        source, target = ((gate_own, gate_got), (up_own, up_got))[kind]
        source = source.at[:, pl.ds(pl.multiple_of(peer * width + first * GROUP, GROUP), span)]
        target = target.at[slot, :, pl.ds(first * GROUP, span)]
        if step == 0:
            return pltpu.make_async_copy(source, target, scale_recv.at[kind, i, slot])
        return remote(
            source, target, scale_send.at[kind], scale_recv.at[kind, i, slot], row=peer
        )

    def down_copy(step):
        peer = lax.rem(row + step, rows)
        if step == 0:
            return pltpu.make_async_copy(
                down_turned.at[peer], down_got.at[slot], down_recv.at[slot]
            )
        return remote(
            down_turned.at[peer], down_got.at[slot], scale_send.at[2], down_recv.at[slot], row=peer
        )

    def start_scales(i):
        @pl.when(home)
        def _():
            for step in range(rows):
                for kind in range(2):
                    scale_copy(kind, i, step).start()

    def wait_slot(copy_of, t, finish):
        here = row == col * share + t

        @pl.when(here)
        def _():
            copy_of(0).wait()

        @pl.when(jnp.logical_not(here))
        def _():
            finish().wait_recv()

    def wait_scales(i):
        first, end = pieces[i]
        at = pl.ds(first * GROUP, (end - first) * GROUP)
        peer = lax.rem(row + 1, rows)
        for t in range(share):
            for kind, target in enumerate((gate_got, up_got)):
                source = (gate_own, up_own)[kind]
                wait_slot(
                    lambda step: scale_copy(kind, i, step),
                    t,
                    lambda: remote(
                        source.at[:, at], target.at[t, :, at], scale_send.at[kind],
                        scale_recv.at[kind, i, t], row=peer,
                    ),
                )

    def wait_down():
        peer = lax.rem(row + 1, rows)
        span = down_got.shape[2]
        for t in range(share):
            wait_slot(
                down_copy,
                t,
                lambda: remote(
                    down_turned.at[0], down_got.at[t], scale_send.at[2], down_recv.at[t], row=peer
                ),
            )
        for t in range(share):
            down_rows[:, t * span : (t + 1) * span] = down_got[t].astype(jnp.float32)

    crossed = exact and chips == 4 and count % 32 == 0
    piece = count // 2

    def token_copy(source, target, peer, slice_index=None):
        def at(j):
            if slice_index is None:
                return block(core, j)
            first = (core * chips + j) * count + slice_index * piece
            return pl.ds(pl.multiple_of(first, piece), piece)

        index = 2 * target + (slice_index or 0)
        return remote(
            all_tokens.at[at(source)], all_tokens.at[at(target)],
            token_send.at[index], token_recv.at[index], row=other(peer) + core,
        )

    def relay(j):
        return remote(
            all_tokens.at[block(core, j)], all_tokens.at[block(core, j)],
            relay_send.at[j], relay_recv.at[j], row=sibling,
        )

    if crossed:
        token_sends = [token_copy(0, j, j, p) for j, p in ((1, 0), (2, 1), (1, 1), (2, 0))]
        token_hands = [token_copy(1, 3, 2, 0), token_copy(2, 3, 1, 1)]
    else:
        token_sends = [token_copy(0, back(j), j) for j in range(chips - 1, 0, -1)]
        token_hands = []

    @pl.when(home)
    def _():
        for load in scale_loads:
            load.wait()

    start_scales(0)
    own_copy.wait()
    def send_scales():
        for i in range(1, len(pieces)):
            start_scales(i)
            for copy in code_copies(i):
                copy.start()

        @pl.when(home)
        def _():
            down_groups = down_own.shape[1] // rows
            line = lax.broadcasted_iota(jnp.int32, (rows * down_got.shape[1], down_own.shape[1]), 0)
            wanted = lax.broadcasted_iota(jnp.int32, line.shape, 1)
            owner = lax.div(line, down_got.shape[1])
            group = lax.rem(line, down_got.shape[1])
            pick = (wanted == owner * down_groups + group) & (group < down_groups)
            turned = lax.dot_general(
                pick.astype(jnp.bfloat16), down_own[...], (((1,), (1,)), ((), ())),
                preferred_element_type=jnp.float32,
            )
            down_turned[...] = turned.astype(jnp.bfloat16).reshape(down_turned.shape)
            for step in range(rows):
                down_copy(step).start()

    for copy in token_sends:
        copy.start()
    relay(0).start()
    down_load = pltpu.make_async_copy(down, down_codes, local_sem.at[1])
    down_load.start()
    acc[...] = jnp.zeros_like(acc)
    batch = 4 if groups % 4 == 0 else 1

    def dequantize_up(t):
        at = pl.ds(pl.multiple_of(t * GROUP, GROUP), GROUP)
        for kind, (codes, scale) in enumerate(((gate_codes, gate_got), (up_codes, up_got))):
            for s in range(share):
                unit_scale[kind, s * lines : (s + 1) * lines, :] = scale[s, :, at].astype(jnp.float32)

        def one(b, carry):
            for kind, codes in enumerate((gate_codes, up_codes)):
                word = codes[pl.ds(pl.multiple_of(b * batch * SUB, SUB), batch * SUB), at] ^ FLIP
                word = word.reshape(batch, SUB, GROUP)
                scale = jnp.stack(
                    [unit_scale[kind, pl.ds(b * batch + i, 1), :] for i in range(batch)]
                )
                for k in range(PACK):
                    value = (nibbles(word, k) * scale).astype(jnp.bfloat16)
                    dense[pl.ds(b * batch, batch), k, :, kind * GROUP : (kind + 1) * GROUP] = value
            return carry

        lax.fori_loop(0, groups // batch, one, 0)

    def ready(i):
        for copy in code_copies(i):
            copy.wait()
        wait_scales(i)

    if crossed:
        for copy, hand in zip(token_sends[:2], token_hands):
            copy.wait_recv()
            hand.start()
        send_scales()
        for j, copy in zip((1, 2), token_sends[2:]):
            copy.wait_recv()
            relay(j).start()
        ready(0)
        dequantize_up(0)
        for hand in token_hands:
            hand.wait_recv()
        relay(3).start()
    else:
        send_scales()
        for j in range(1, chips):
            token_copy(0, j, back(j)).wait_recv()
            relay(j).start()
        ready(0)
        dequantize_up(0)
    for j in range(chips):
        relay(j).wait_recv()

    rows_step = min(total_tokens, 256)
    perm = permutation()

    def permute(i, carry):
        lines_at = pl.ds(pl.multiple_of(i * rows_step, rows_step), rows_step)
        for group in range(model // GROUP):
            at = pl.ds(group * GROUP, GROUP)
            moved[lines_at, at] = jnp.dot(
                all_tokens[lines_at, at], perm, preferred_element_type=jnp.float32
            ).astype(jnp.bfloat16)
        return carry

    lax.fori_loop(0, total_tokens // rows_step, permute, 0)

    def multiply_up(t):
        def multiply(i, carry):
            lines_at = pl.ds(pl.multiple_of(i * rows_step, rows_step), rows_step)
            total = jnp.dot(
                moved[lines_at, :],
                dense[...].reshape(model, 2 * GROUP),
                preferred_element_type=jnp.float32,
            )
            sums[t, lines_at, :] = total.astype(jnp.bfloat16)
            return carry

        lax.fori_loop(0, total_tokens // rows_step, multiply, 0)

    def side_rows(side):
        return pl.ds(side * half, half)

    def sum_copy(side, q, p, source, peer):
        at = pl.ds(p * part, part)
        index = q * PARTS + p
        return remote(
            source, got.at[side, q, at], sum_send.at[side], sum_recv.at[side, index], col=peer
        )

    per_chip = chunks // quad
    steps = chips * per_chip

    early = min(EARLY, per_chip - 1)
    late = per_chip - early

    def piece_of(tau):
        rest = tau - chips * early
        soon = rest < 0
        j = jnp.where(soon, lax.rem(tau, chips), lax.div(jnp.maximum(rest, 0), late))
        k = jnp.where(
            soon, lax.div(tau, chips), early + lax.rem(jnp.maximum(rest, 0), late)
        )
        return chips - 1 - j, k * quad

    def hid_copy(side, tau, peer):
        j, first = piece_of(tau)
        ref = hidden.at[side, j, pl.ds(first, quad)]
        return remote(ref, ref, hid_send.at[side], hid_recv.at[side, tau], col=peer)

    h_start = last * S_LAG + H_WAIT + max(quad - 1, chunks - chips * early - late)
    d_start = h_start + last * H_LAG

    before, after = jnp.maximum(col - 1, 0), jnp.minimum(col + 1, last)
    any_peer = jnp.where(col == last, col - 1, col + 1)
    sides = ((col, after, before), (last - col, before, after))

    def dequantize_down(group):
        word = down_codes[pl.ds(pl.multiple_of(group * SUB, SUB), SUB), :] ^ FLIP
        scale = down_rows[pl.ds(group, 1), :]
        for k in range(PACK):
            dense_down[group, k] = (nibbles(word, k) * scale).astype(jnp.bfloat16)

    columns = 512 if model % 512 == 0 else GROUP

    def multiply_down(tau):
        j, first = piece_of(tau)
        left = jnp.concatenate(
            [hidden[:, j, first + c].reshape(2 * count, GROUP) for c in range(quad)], axis=1
        )
        for n in range(0, model, columns):
            at = pl.ds(n, columns)
            right = dense_down[pl.ds(first, quad), :, :, at].reshape(quad * GROUP, columns)
            total = jnp.dot(left, right, preferred_element_type=jnp.float32)
            acc[j, :, :, at] += total.reshape(2, count, columns)

    def half_copy(j):
        return remote(
            half_send.at[j], half_got.at[j], half_ssem.at[j], half_rsem.at[j], row=sibling
        )

    def final_copy(j, target):
        return remote(
            comb.at[j], final_got.at[target], final_ssem.at[j], final_rsem.at[target],
            row=other(j) + core,
        )

    def give_sibling(j):
        half_send[j] = acc[j, 1 - core].astype(jnp.bfloat16)
        half_copy(j).start()

    def give_chip(j):
        half_copy(j).wait_recv()
        comb[j] = (acc[j, core] + half_got[j].astype(jnp.float32)).astype(jnp.bfloat16)
        final_copy(j, back(j)).start()

    def sent_early():
        for copy in token_sends + token_hands:
            copy.wait_send()
        for j in range(chips):
            relay(j).wait_send()

        @pl.when(home)
        def _():
            most = pl.ds(0, (rows - 1) * width)
            for kind, ref in enumerate((gate_own.at[:, most], up_own.at[:, most])):
                remote(
                    ref, ref, scale_send.at[kind], scale_recv.at[kind, 0, 0], row=sibling
                ).wait_send()
            ref = down_turned.at[pl.ds(0, rows - 1)]
            remote(ref, ref, scale_send.at[2], down_recv.at[0], row=sibling).wait_send()

    def tick(t, carry):
        @pl.when(t < chunks)
        def _():
            multiply_up(t)
            for side, (hops, onward, backward) in enumerate(sides):
                @pl.when(hops == 0)
                def _():
                    for p in range(PARTS):
                        own = sums.at[t, pl.ds(side * half + p * part, part)]
                        sum_copy(side, t, p, own, onward).start()

        for i, (first, end) in enumerate(pieces[1:], 1):
            @pl.when(t + 1 == first)
            def _():
                ready(i)

        @pl.when(t + 1 < chunks)
        def _():
            dequantize_up(t + 1)

        for side, (hops, onward, backward) in enumerate(sides):
            q = t - S_LAG * hops

            @pl.when((hops > 0) & (q >= 0) & (q < chunks))
            def _():
                @pl.when(hops < last)
                def _():
                    for p in range(PARTS):
                        at = pl.ds(p * part, part)
                        own = sums[q, pl.ds(side * half + p * part, part), :]
                        sum_copy(side, q, p, got.at[side, q, at], any_peer).wait_recv()
                        total = got[side, q, at, :].astype(jnp.float32) + own.astype(jnp.float32)
                        got[side, q, at, :] = total.astype(jnp.bfloat16)
                        sum_copy(side, q, p, got.at[side, q, at], onward).start()

                @pl.when(hops == last)
                def _():
                    for p in range(PARTS):
                        at = pl.ds(p * part, part)
                        sum_copy(side, q, p, got.at[side, q, at], any_peer).wait_recv()
                    total = got[side, q].astype(jnp.float32) + sums[
                        q, side_rows(side), :
                    ].astype(jnp.float32)
                    value = jax.nn.silu(total[:, :GROUP]) * total[:, GROUP:]
                    value = jnp.dot(
                        value.astype(jnp.bfloat16), perm, preferred_element_type=jnp.float32
                    ).astype(jnp.bfloat16)
                    for j in range(chips):
                        hidden[side, j, q] = value[j * count : (j + 1) * count]

        group = (t - chunks) * pair

        @pl.when(group == 0)
        def _():
            down_load.wait()
            wait_down()

        @pl.when((group >= 0) & (group < chunks))
        def _():
            for i in range(pair):
                dequantize_down(group + i)

        for side, (hops, onward, backward) in enumerate(sides):
            left = last - hops
            tau = t - h_start - H_LAG * left

            @pl.when((tau >= 0) & (tau < steps))
            def _():
                @pl.when(left > 0)
                def _():
                    hid_copy(side, tau, any_peer).wait_recv()

                @pl.when(left < last)
                def _():
                    hid_copy(side, tau, backward).start()

        tau = t - d_start

        @pl.when(tau >= 0)
        def _():
            multiply_down(tau)

        for j in range(chips - 1, 0, -1):
            done = chips * early + (chips - j) * late

            @pl.when(tau == done - 1)
            def _():
                give_sibling(j)

            @pl.when(tau == done + min(1, late - 1))
            def _():
                give_chip(j)

        @pl.when(t == chunks)
        def _():
            sent_early()

        return carry

    lax.fori_loop(0, d_start + steps, tick, 0)

    half_send[0] = acc[0, 1 - core].astype(jnp.bfloat16)
    half_copy(0).start()
    total = acc[0, core]
    for j in range(1, chips):
        final_copy(back(j), j).wait_recv()
        total = total + final_got[j].astype(jnp.float32)
    half_copy(0).wait_recv()
    out[...] = (total + half_got[0].astype(jnp.float32)).astype(jnp.bfloat16)

    for j in range(1, chips):
        final_copy(j, back(j)).wait_send()
    for j in range(chips):
        half_copy(j).wait_send()
    for side, (hops, onward, backward) in enumerate(sides):
        @pl.when(hops < last)
        def _():
            ref = got.at[side]
            remote(ref, ref, sum_send.at[side], sum_recv.at[side, 0], col=any_peer).wait_send()

        @pl.when(hops > 0)
        def _():
            ref = hidden.at[side]
            remote(ref, ref, hid_send.at[side], hid_recv.at[side, 0], col=any_peer).wait_send()


def layer(tokens, gate, up, down, gate_scale, up_scale, down_scale, rows, cols):
    count, model = tokens.shape
    words, width = gate.shape
    lines = gate_scale.shape[0]
    share = rows // cols
    down_groups = down_scale.shape[1] // rows
    span = down_scale.shape[0]
    lines_down = -(-down_groups // 16) * 16
    chunks = width // GROUP
    chips = rows // 2
    tokens_all = count * rows
    half = tokens_all // 2
    groups = share * lines
    pair, quad = 2 - chunks % 2, 4 if chunks % 4 == 0 else 1
    steps = chips * (chunks // quad)
    parts = len(pieces_of(chunks))
    any_spec = pl.BlockSpec(memory_space=pl.ANY)
    bf16, f32, i32 = jnp.bfloat16, jnp.float32, jnp.int32
    return pl.pallas_call(
        functools.partial(layer_kernel, rows, cols, chunks),
        in_specs=[any_spec] * 7,
        out_specs=pl.BlockSpec(memory_space=pltpu.VMEM),
        out_shape=jax.ShapeDtypeStruct((count, model), bf16),
        scratch_shapes=[
            pltpu.VMEM((tokens_all, model), bf16),
            pltpu.VMEM((tokens_all, model), bf16),
            pltpu.VMEM((words, width), i32),
            pltpu.VMEM((words, width), i32),
            pltpu.VMEM(down.shape, i32),
            pltpu.VMEM(gate_scale.shape, bf16),
            pltpu.VMEM(up_scale.shape, bf16),
            pltpu.VMEM(down_scale.shape, bf16),
            pltpu.VMEM((rows, lines_down, span), bf16),
            pltpu.VMEM((share, lines, width), bf16),
            pltpu.VMEM((share, lines, width), bf16),
            pltpu.VMEM((share, lines_down, span), bf16),
            pltpu.VMEM((2, groups, GROUP), f32),
            pltpu.VMEM((lines_down, share * span), f32),
            pltpu.VMEM((groups, PACK, SUB, 2 * GROUP), bf16),
            pltpu.VMEM((chunks, PACK, SUB, model), bf16),
            pltpu.VMEM((chunks, tokens_all, 2 * GROUP), bf16),
            pltpu.VMEM((2, chunks, half, 2 * GROUP), bf16),
            pltpu.VMEM((2, chips, chunks, count, GROUP), bf16),
            pltpu.VMEM((chips, 2, count, model), f32),
            pltpu.VMEM((chips, count, model), bf16),
            pltpu.VMEM((chips, count, model), bf16),
            pltpu.VMEM((chips, count, model), bf16),
            pltpu.VMEM((chips, count, model), bf16),
            DMA((5 + 2 * parts,)),
            DMA((2 * chips,)),
            DMA((2 * chips,)),
            DMA((chips,)),
            DMA((chips,)),
            DMA((3,)),
            DMA((2, parts, share)),
            DMA((share,)),
            DMA((2,)),
            DMA((2, chunks * PARTS)),
            DMA((2,)),
            DMA((2, steps)),
            DMA((chips,)),
            DMA((chips,)),
            DMA((chips,)),
            DMA((chips,)),
        ],
        compiler_params=pltpu.CompilerParams(
            collective_id=0, has_side_effects=True, vmem_limit_bytes=60 * 1024 * 1024
        ),
        name="layer",
    )(tokens, gate, up, down, gate_scale, up_scale, down_scale)


def per_device(tokens, gate_codes, up_codes, down_codes, gate_scales, up_scales, down_scales):
    rows, cols = lax.axis_size("row"), lax.axis_size("col")
    return layer(
        tokens, gate_codes, up_codes, down_codes, gate_scales, up_scales, down_scales, rows, cols
    )


def solution(mesh):
    placed = (
        P("row", "col"),
        P("col", "row"),
        P("col", "row"),
        P("row", "col"),
        P("row", None),
        P("row", None),
        P("row", None),
    )
    return jax.shard_map(
        per_device, mesh=mesh, in_specs=placed, out_specs=P("row", "col"), check_vma=False
    )
```

```python
import functools

import jax
import jax.numpy as jnp
from jax import lax
from jax.experimental import pallas as pl
from jax.experimental.pallas import tpu as pltpu
from jax.sharding import PartitionSpec as P

GROUP = 128
PACK = 8
SUB = GROUP // PACK
MESH = pl.DeviceIdType.MESH
DMA = pltpu.SemaphoreType.DMA
S_LAG = 3
H_LAG = 5
H_WAIT = 0
PARTS = 1
EARLY = 1
FLIP = -2004318072


def permutation():
    source = lax.broadcasted_iota(jnp.int32, (GROUP, GROUP), 0)
    target = lax.broadcasted_iota(jnp.int32, (GROUP, GROUP), 1)
    wanted = lax.rem(target, SUB) * PACK + lax.div(target, SUB)
    return (source == wanted).astype(jnp.bfloat16)


def pieces_of(chunks):
    bounds = sorted({0, 1, max(1, chunks // 7), max(1, 3 * chunks // 7), chunks})
    return list(zip(bounds[:-1], bounds[1:]))


def nibbles(word, k):
    code = word if k == PACK - 1 else jnp.left_shift(word, 28 - 4 * k)
    return jnp.right_shift(code, 28).astype(jnp.float32)


def layer_kernel(
    rows, cols, chunks,
    tokens, gate, up, down, gate_scale, up_scale, down_scale, out,
    all_tokens, moved, gate_codes, up_codes, down_codes,
    gate_own, up_own, down_own, down_turned,
    gate_got, up_got, down_got, unit_scale, down_rows,
    dense, dense_down, sums, got,
    hidden, acc,
    half_send, half_got, comb, final_got,
    local_sem, token_send, token_recv, relay_send, relay_recv,
    scale_send, scale_recv, down_recv,
    sum_send, sum_recv, hid_send, hid_recv,
    half_ssem, half_rsem, final_ssem, final_rsem,
):
    row, col = lax.axis_index("row"), lax.axis_index("col")
    core = lax.rem(row, 2)
    chip = row - core
    sibling = row + 1 - 2 * core
    chips = rows // 2
    share = rows // cols
    last = cols - 1
    count, model = tokens.shape
    total_tokens = count * rows
    half = total_tokens // 2
    width = gate.shape[1]
    lines = gate_scale.shape[0]
    groups = share * lines
    part = half // PARTS
    pair, quad = 2 - chunks % 2, 4 if chunks % 4 == 0 else 1
    pieces = pieces_of(chunks)
    home = lax.div(row, share) == col
    slot = lax.rem(row, share)
    exact = chips & (chips - 1) == 0

    def other(j):
        if not exact:
            return lax.rem(chip + 2 * j, rows)
        peer, bit = chip, 2
        while bit <= 2 * j:
            if (2 * j) & bit:
                peer = peer + bit - 2 * bit * lax.rem(lax.div(chip, bit), 2)
            bit *= 2
        return peer

    def back(j):
        return j if exact else (chips - j) % chips

    def block(side, j):
        return pl.ds(pl.multiple_of((side * chips + j) * count, count), count)

    def remote(source, target, send, recv, **where):
        return pltpu.make_async_remote_copy(
            src_ref=source, dst_ref=target, send_sem=send, recv_sem=recv,
            device_id=where, device_id_type=MESH,
        )

    own_copy = pltpu.make_async_copy(tokens, all_tokens.at[block(core, 0)], local_sem.at[0])
    own_copy.start()

    def code_copies(i):
        first, end = pieces[i]
        at = pl.ds(first * GROUP, (end - first) * GROUP)
        return [
            pltpu.make_async_copy(gate.at[:, at], gate_codes.at[:, at], local_sem.at[2 + 2 * i]),
            pltpu.make_async_copy(up.at[:, at], up_codes.at[:, at], local_sem.at[3 + 2 * i]),
        ]

    for copy in code_copies(0):
        copy.start()
    first_code = 2 + 2 * len(pieces)
    scale_loads = [
        pltpu.make_async_copy(source, target, local_sem.at[first_code + i])
        for i, (source, target) in enumerate(
            ((gate_scale, gate_own), (up_scale, up_own), (down_scale, down_own))
        )
    ]

    @pl.when(home)
    def _():
        for load in scale_loads:
            load.start()

    barrier = pltpu.get_barrier_semaphore()
    for step in range(1, rows):
        pl.semaphore_signal(
            barrier, inc=1, device_id={"row": lax.rem(row + step, rows)}, device_id_type=MESH
        )

    @pl.when(col > 0)
    def _():
        pl.semaphore_signal(barrier, inc=1, device_id={"col": col - 1}, device_id_type=MESH)

    @pl.when(col < last)
    def _():
        pl.semaphore_signal(barrier, inc=1, device_id={"col": col + 1}, device_id_type=MESH)

    inner = jnp.logical_and(col > 0, col < last)

    @pl.when(inner)
    def _():
        pl.semaphore_wait(barrier, rows + 1)

    @pl.when(jnp.logical_not(inner))
    def _():
        pl.semaphore_wait(barrier, rows)

    def scale_copy(kind, i, step):
        first, end = pieces[i]
        peer = lax.rem(row + step, rows)
        span = (end - first) * GROUP
        source, target = ((gate_own, gate_got), (up_own, up_got))[kind]
        source = source.at[:, pl.ds(pl.multiple_of(peer * width + first * GROUP, GROUP), span)]
        target = target.at[slot, :, pl.ds(first * GROUP, span)]
        if step == 0:
            return pltpu.make_async_copy(source, target, scale_recv.at[kind, i, slot])
        return remote(
            source, target, scale_send.at[kind], scale_recv.at[kind, i, slot], row=peer
        )

    def down_copy(step):
        peer = lax.rem(row + step, rows)
        if step == 0:
            return pltpu.make_async_copy(
                down_turned.at[peer], down_got.at[slot], down_recv.at[slot]
            )
        return remote(
            down_turned.at[peer], down_got.at[slot], scale_send.at[2], down_recv.at[slot], row=peer
        )

    def start_scales(i):
        @pl.when(home)
        def _():
            for step in range(rows):
                for kind in range(2):
                    scale_copy(kind, i, step).start()

    def wait_slot(copy_of, t, finish):
        here = row == col * share + t

        @pl.when(here)
        def _():
            copy_of(0).wait()

        @pl.when(jnp.logical_not(here))
        def _():
            finish().wait_recv()

    def wait_scales(i):
        first, end = pieces[i]
        at = pl.ds(first * GROUP, (end - first) * GROUP)
        peer = lax.rem(row + 1, rows)
        for t in range(share):
            for kind, target in enumerate((gate_got, up_got)):
                source = (gate_own, up_own)[kind]
                wait_slot(
                    lambda step: scale_copy(kind, i, step),
                    t,
                    lambda: remote(
                        source.at[:, at], target.at[t, :, at], scale_send.at[kind],
                        scale_recv.at[kind, i, t], row=peer,
                    ),
                )

    def wait_down():
        peer = lax.rem(row + 1, rows)
        span = down_got.shape[2]
        for t in range(share):
            wait_slot(
                down_copy,
                t,
                lambda: remote(
                    down_turned.at[0], down_got.at[t], scale_send.at[2], down_recv.at[t], row=peer
                ),
            )
        for t in range(share):
            down_rows[:, t * span : (t + 1) * span] = down_got[t].astype(jnp.float32)

    crossed = exact and chips == 4 and count % 32 == 0 and model % (2 * GROUP) == 0
    piece = count // 2

    def token_copy(source, target, peer, slice_index=None, lane=0):
        lanes = slice(None) if slice_index is None else pl.ds(lane * (model // 2), model // 2)

        def at(j):
            if slice_index is None:
                return block(core, j)
            first = (core * chips + j) * count + slice_index * piece
            return pl.ds(pl.multiple_of(first, piece), piece)

        index = 4 * target + 2 * (slice_index or 0) + lane
        return remote(
            all_tokens.at[at(source), lanes], all_tokens.at[at(target), lanes],
            token_send.at[index], token_recv.at[index], row=other(peer) + core,
        )

    def relay(j):
        return remote(
            all_tokens.at[block(core, j)], all_tokens.at[block(core, j)],
            relay_send.at[j], relay_recv.at[j], row=sibling,
        )

    if crossed:
        token_sends = [
            token_copy(0, j, j, p, lane)
            for order in (((1, 0), (2, 1)), ((1, 1), (2, 0)))
            for lane in range(2)
            for j, p in order
        ]
        token_hands = [
            token_copy(j, 3, 3 - j, j - 1, lane) for lane in range(2) for j in (1, 2)
        ]
    else:
        token_sends = [token_copy(0, back(j), j) for j in range(chips - 1, 0, -1)]
        token_hands = []

    @pl.when(home)
    def _():
        for load in scale_loads:
            load.wait()

    start_scales(0)
    own_copy.wait()
    def send_soon():
        start_scales(1)
        for copy in code_copies(1):
            copy.start()

    def send_scales():
        for i in range(2, len(pieces)):
            start_scales(i)
            for copy in code_copies(i):
                copy.start()

        @pl.when(home)
        def _():
            down_groups = down_own.shape[1] // rows
            line = lax.broadcasted_iota(jnp.int32, (rows * down_got.shape[1], down_own.shape[1]), 0)
            wanted = lax.broadcasted_iota(jnp.int32, line.shape, 1)
            owner = lax.div(line, down_got.shape[1])
            group = lax.rem(line, down_got.shape[1])
            pick = (wanted == owner * down_groups + group) & (group < down_groups)
            turned = lax.dot_general(
                pick.astype(jnp.bfloat16), down_own[...], (((1,), (1,)), ((), ())),
                preferred_element_type=jnp.float32,
            )
            down_turned[...] = turned.astype(jnp.bfloat16).reshape(down_turned.shape)
            for step in range(rows):
                down_copy(step).start()

    for copy in token_sends:
        copy.start()
    relay(0).start()
    down_load = pltpu.make_async_copy(down, down_codes, local_sem.at[1])
    down_load.start()
    acc[...] = jnp.zeros_like(acc)
    batch = 4 if groups % 4 == 0 else 1

    def dequantize_up(t):
        at = pl.ds(pl.multiple_of(t * GROUP, GROUP), GROUP)
        for kind, (codes, scale) in enumerate(((gate_codes, gate_got), (up_codes, up_got))):
            for s in range(share):
                unit_scale[kind, s * lines : (s + 1) * lines, :] = scale[s, :, at].astype(jnp.float32)

        def one(b, carry):
            for kind, codes in enumerate((gate_codes, up_codes)):
                word = codes[pl.ds(pl.multiple_of(b * batch * SUB, SUB), batch * SUB), at] ^ FLIP
                word = word.reshape(batch, SUB, GROUP)
                scale = jnp.stack(
                    [unit_scale[kind, pl.ds(b * batch + i, 1), :] for i in range(batch)]
                )
                for k in range(PACK):
                    value = (nibbles(word, k) * scale).astype(jnp.bfloat16)
                    dense[pl.ds(b * batch, batch), k, :, kind * GROUP : (kind + 1) * GROUP] = value
            return carry

        lax.fori_loop(0, groups // batch, one, 0)

    def ready(i):
        for copy in code_copies(i):
            copy.wait()
        wait_scales(i)

    if crossed:
        for copy, hand in zip(token_sends[:4], token_hands):
            copy.wait_recv()
            hand.start()
        send_soon()
        for copy in token_sends[4:]:
            copy.wait_recv()
        relay(1).start()
        relay(2).start()
        ready(0)
        dequantize_up(0)
        for hand in token_hands:
            hand.wait_recv()
        relay(3).start()
        send_scales()
    else:
        send_soon()
        send_scales()
        for j in range(1, chips):
            token_copy(0, j, back(j)).wait_recv()
            relay(j).start()
        ready(0)
        dequantize_up(0)
    for j in range(chips):
        relay(j).wait_recv()

    rows_step = min(total_tokens, 256)
    perm = permutation()

    def permute(i, carry):
        lines_at = pl.ds(pl.multiple_of(i * rows_step, rows_step), rows_step)
        for group in range(model // GROUP):
            at = pl.ds(group * GROUP, GROUP)
            moved[lines_at, at] = jnp.dot(
                all_tokens[lines_at, at], perm, preferred_element_type=jnp.float32
            ).astype(jnp.bfloat16)
        return carry

    lax.fori_loop(0, total_tokens // rows_step, permute, 0)

    def multiply_up(t):
        def multiply(i, carry):
            lines_at = pl.ds(pl.multiple_of(i * rows_step, rows_step), rows_step)
            total = jnp.dot(
                moved[lines_at, :],
                dense[...].reshape(model, 2 * GROUP),
                preferred_element_type=jnp.float32,
            )
            sums[t, lines_at, :] = total.astype(jnp.bfloat16)
            return carry

        lax.fori_loop(0, total_tokens // rows_step, multiply, 0)

    def side_rows(side):
        return pl.ds(side * half, half)

    def sum_copy(side, q, p, source, peer):
        at = pl.ds(p * part, part)
        index = q * PARTS + p
        return remote(
            source, got.at[side, q, at], sum_send.at[side], sum_recv.at[side, index], col=peer
        )

    per_chip = chunks // quad
    steps = chips * per_chip

    early = min(EARLY, per_chip - 1)
    late = per_chip - early

    def piece_of(tau):
        rest = tau - chips * early
        soon = rest < 0
        j = jnp.where(soon, lax.rem(tau, chips), lax.div(jnp.maximum(rest, 0), late))
        k = jnp.where(
            soon, lax.div(tau, chips), early + lax.rem(jnp.maximum(rest, 0), late)
        )
        return chips - 1 - j, k * quad

    def hid_copy(side, tau, peer):
        j, first = piece_of(tau)
        ref = hidden.at[side, j, pl.ds(first, quad)]
        return remote(ref, ref, hid_send.at[side], hid_recv.at[side, tau], col=peer)

    h_start = last * S_LAG + H_WAIT + max(quad - 1, chunks - chips * early - late)
    d_start = h_start + last * H_LAG

    before, after = jnp.maximum(col - 1, 0), jnp.minimum(col + 1, last)
    any_peer = jnp.where(col == last, col - 1, col + 1)
    sides = ((col, after, before), (last - col, before, after))

    def dequantize_down(group):
        word = down_codes[pl.ds(pl.multiple_of(group * SUB, SUB), SUB), :] ^ FLIP
        scale = down_rows[pl.ds(group, 1), :]
        for k in range(PACK):
            dense_down[group, k] = (nibbles(word, k) * scale).astype(jnp.bfloat16)

    columns = 512 if model % 512 == 0 else GROUP

    def multiply_down(first, j, size):
        left = jnp.concatenate(
            [
                hidden[:, pl.ds(j, size), first + c].reshape(2 * size * count, GROUP)
                for c in range(quad)
            ],
            axis=1,
        )
        for n in range(0, model, columns):
            at = pl.ds(n, columns)
            right = dense_down[pl.ds(first, quad), :, :, at].reshape(quad * GROUP, columns)
            total = jnp.dot(left, right, preferred_element_type=jnp.float32)
            acc[:, pl.ds(j, size), :, at] += total.reshape(2, size, count, columns)

    def half_copy(j):
        return remote(
            half_send.at[j], half_got.at[j], half_ssem.at[j], half_rsem.at[j], row=sibling
        )

    def final_copy(j, target):
        return remote(
            comb.at[j], final_got.at[target], final_ssem.at[j], final_rsem.at[target],
            row=other(j) + core,
        )

    def give_sibling(j):
        half_send[j] = acc[1 - core, j].astype(jnp.bfloat16)
        half_copy(j).start()

    def give_chip(j):
        half_copy(j).wait_recv()
        comb[j] = (acc[core, j] + half_got[j].astype(jnp.float32)).astype(jnp.bfloat16)
        final_copy(j, back(j)).start()

    def sent_early():
        for copy in token_sends + token_hands:
            copy.wait_send()
        for j in range(chips):
            relay(j).wait_send()

        @pl.when(home)
        def _():
            most = pl.ds(0, (rows - 1) * width)
            for kind, ref in enumerate((gate_own.at[:, most], up_own.at[:, most])):
                remote(
                    ref, ref, scale_send.at[kind], scale_recv.at[kind, 0, 0], row=sibling
                ).wait_send()
            ref = down_turned.at[pl.ds(0, rows - 1)]
            remote(ref, ref, scale_send.at[2], down_recv.at[0], row=sibling).wait_send()

    def tick(t, carry):
        @pl.when(t < chunks)
        def _():
            multiply_up(t)
            for side, (hops, onward, backward) in enumerate(sides):
                @pl.when(hops == 0)
                def _():
                    for p in range(PARTS):
                        own = sums.at[t, pl.ds(side * half + p * part, part)]
                        sum_copy(side, t, p, own, onward).start()

        for i, (first, end) in enumerate(pieces[1:], 1):
            @pl.when(t + 1 == first)
            def _():
                ready(i)

        @pl.when(t + 1 < chunks)
        def _():
            dequantize_up(t + 1)

        for side, (hops, onward, backward) in enumerate(sides):
            q = t - S_LAG * hops

            @pl.when((hops > 0) & (q >= 0) & (q < chunks))
            def _():
                @pl.when(hops < last)
                def _():
                    for p in range(PARTS):
                        at = pl.ds(p * part, part)
                        own = sums[q, pl.ds(side * half + p * part, part), :]
                        sum_copy(side, q, p, got.at[side, q, at], any_peer).wait_recv()
                        total = got[side, q, at, :].astype(jnp.float32) + own.astype(jnp.float32)
                        got[side, q, at, :] = total.astype(jnp.bfloat16)
                        sum_copy(side, q, p, got.at[side, q, at], onward).start()

                @pl.when(hops == last)
                def _():
                    for p in range(PARTS):
                        at = pl.ds(p * part, part)
                        sum_copy(side, q, p, got.at[side, q, at], any_peer).wait_recv()
                    total = got[side, q].astype(jnp.float32) + sums[
                        q, side_rows(side), :
                    ].astype(jnp.float32)
                    value = jax.nn.silu(total[:, :GROUP]) * total[:, GROUP:]
                    value = jnp.dot(
                        value.astype(jnp.bfloat16), perm, preferred_element_type=jnp.float32
                    ).astype(jnp.bfloat16)
                    for j in range(chips):
                        hidden[side, j, q] = value[j * count : (j + 1) * count]

        group = (t - chunks) * pair

        @pl.when(group == 0)
        def _():
            down_load.wait()
            wait_down()

        @pl.when((group >= 0) & (group < chunks))
        def _():
            for i in range(pair):
                dequantize_down(group + i)

        for side, (hops, onward, backward) in enumerate(sides):
            left = last - hops
            tau = t - h_start - H_LAG * left

            @pl.when((tau >= 0) & (tau < steps))
            def _():
                @pl.when(left > 0)
                def _():
                    hid_copy(side, tau, any_peer).wait_recv()

                @pl.when(left < last)
                def _():
                    hid_copy(side, tau, backward).start()

        tau = t - d_start

        j, first = piece_of(jnp.maximum(tau, 0))
        soon = tau < chips * early

        @pl.when((tau >= 0) & soon & (j == 0))
        def _():
            multiply_down(first, 0, chips)

        @pl.when(jnp.logical_not(soon) & (j == chips - 2))
        def _():
            multiply_down(first, chips - 2, 2)

        @pl.when(jnp.logical_not(soon) & (j < chips - 2))
        def _():
            multiply_down(first, j, 1)

        for j in range(chips - 1, 0, -1):
            done = chips * early + (chips - min(j, chips - 2)) * late

            @pl.when(tau == done - 1)
            def _():
                give_sibling(j)

            @pl.when(tau == done + min(1, late - 1))
            def _():
                give_chip(j)

        @pl.when(t == chunks)
        def _():
            sent_early()

        return carry

    lax.fori_loop(0, d_start + steps, tick, 0)

    half_send[0] = acc[1 - core, 0].astype(jnp.bfloat16)
    half_copy(0).start()
    total = acc[core, 0]
    for j in range(1, chips):
        final_copy(back(j), j).wait_recv()
        total = total + final_got[j].astype(jnp.float32)
    half_copy(0).wait_recv()
    out[...] = (total + half_got[0].astype(jnp.float32)).astype(jnp.bfloat16)

    for j in range(1, chips):
        final_copy(j, back(j)).wait_send()
    for j in range(chips):
        half_copy(j).wait_send()
    for side, (hops, onward, backward) in enumerate(sides):
        @pl.when(hops < last)
        def _():
            ref = got.at[side]
            remote(ref, ref, sum_send.at[side], sum_recv.at[side, 0], col=any_peer).wait_send()

        @pl.when(hops > 0)
        def _():
            ref = hidden.at[side]
            remote(ref, ref, hid_send.at[side], hid_recv.at[side, 0], col=any_peer).wait_send()


def layer(tokens, gate, up, down, gate_scale, up_scale, down_scale, rows, cols):
    count, model = tokens.shape
    words, width = gate.shape
    lines = gate_scale.shape[0]
    share = rows // cols
    down_groups = down_scale.shape[1] // rows
    span = down_scale.shape[0]
    lines_down = -(-down_groups // 16) * 16
    chunks = width // GROUP
    chips = rows // 2
    tokens_all = count * rows
    half = tokens_all // 2
    groups = share * lines
    pair, quad = 2 - chunks % 2, 4 if chunks % 4 == 0 else 1
    steps = chips * (chunks // quad)
    parts = len(pieces_of(chunks))
    any_spec = pl.BlockSpec(memory_space=pl.ANY)
    bf16, f32, i32 = jnp.bfloat16, jnp.float32, jnp.int32
    return pl.pallas_call(
        functools.partial(layer_kernel, rows, cols, chunks),
        in_specs=[any_spec] * 7,
        out_specs=pl.BlockSpec(memory_space=pltpu.VMEM),
        out_shape=jax.ShapeDtypeStruct((count, model), bf16),
        scratch_shapes=[
            pltpu.VMEM((tokens_all, model), bf16),
            pltpu.VMEM((tokens_all, model), bf16),
            pltpu.VMEM((words, width), i32),
            pltpu.VMEM((words, width), i32),
            pltpu.VMEM(down.shape, i32),
            pltpu.VMEM(gate_scale.shape, bf16),
            pltpu.VMEM(up_scale.shape, bf16),
            pltpu.VMEM(down_scale.shape, bf16),
            pltpu.VMEM((rows, lines_down, span), bf16),
            pltpu.VMEM((share, lines, width), bf16),
            pltpu.VMEM((share, lines, width), bf16),
            pltpu.VMEM((share, lines_down, span), bf16),
            pltpu.VMEM((2, groups, GROUP), f32),
            pltpu.VMEM((lines_down, share * span), f32),
            pltpu.VMEM((groups, PACK, SUB, 2 * GROUP), bf16),
            pltpu.VMEM((chunks, PACK, SUB, model), bf16),
            pltpu.VMEM((chunks, tokens_all, 2 * GROUP), bf16),
            pltpu.VMEM((2, chunks, half, 2 * GROUP), bf16),
            pltpu.VMEM((2, chips, chunks, count, GROUP), bf16),
            pltpu.VMEM((2, chips, count, model), f32),
            pltpu.VMEM((chips, count, model), bf16),
            pltpu.VMEM((chips, count, model), bf16),
            pltpu.VMEM((chips, count, model), bf16),
            pltpu.VMEM((chips, count, model), bf16),
            DMA((5 + 2 * parts,)),
            DMA((4 * chips,)),
            DMA((4 * chips,)),
            DMA((chips,)),
            DMA((chips,)),
            DMA((3,)),
            DMA((2, parts, share)),
            DMA((share,)),
            DMA((2,)),
            DMA((2, chunks * PARTS)),
            DMA((2,)),
            DMA((2, steps)),
            DMA((chips,)),
            DMA((chips,)),
            DMA((chips,)),
            DMA((chips,)),
        ],
        compiler_params=pltpu.CompilerParams(
            collective_id=0, has_side_effects=True, vmem_limit_bytes=60 * 1024 * 1024
        ),
        name="layer",
    )(tokens, gate, up, down, gate_scale, up_scale, down_scale)


def per_device(tokens, gate_codes, up_codes, down_codes, gate_scales, up_scales, down_scales):
    rows, cols = lax.axis_size("row"), lax.axis_size("col")
    return layer(
        tokens, gate_codes, up_codes, down_codes, gate_scales, up_scales, down_scales, rows, cols
    )


def solution(mesh):
    placed = (
        P("row", "col"),
        P("col", "row"),
        P("col", "row"),
        P("row", "col"),
        P("row", None),
        P("row", None),
        P("row", None),
    )
    return jax.shard_map(
        per_device, mesh=mesh, in_specs=placed, out_specs=P("row", "col"), check_vma=False
    )
```
